32 devices in a mesh: fsdp: 2 (over y), tensor: 16 (over z, x, core).
Axes of the slice: x: 2, y: 2, z: 4, core: 2. Of those that a mesh axis runs over, the one named last changes fastest.
Arguments:
- momentum: bfloat16 [8192, 28672], P('fsdp', 'tensor'), may hold values from -6 to 6
- gradient: bfloat16 [8192, 28672], P('fsdp', 'tensor'), may hold values from -4 to 4
- factor: float32 [28672, 512], P('tensor', 'fsdp'), may hold values from -0.03125 to 0.03125
Outputs:
- new_momentum: bfloat16 [8192, 28672], P('fsdp', 'tensor')
- new_factor: float32 [28672, 512], P('tensor', 'fsdp')
- update: bfloat16 [8192, 28672], P('fsdp', 'tensor')
The draws below stay inside these ranges and needn't reach their ends.
All inputs are finite; a program needn't handle non-finite values.
Results may differ from the reference program's by a relative error of at most 0.017.
Values may be sent and summed in bfloat16 or wider, within the bound.
A program may use at most 128 MiB of HBM per device.

```python
import jax
import jax.numpy as jnp
from jax import lax

D = 8192
FF = 28672
R = 512


def steps_of(own_key, shape, shards, smallest, top_value):
    level = 1.0
    for dim, parts in shards:
        heights = jax.random.uniform(jax.random.fold_in(jax.random.fold_in(own_key, 6), dim), (parts,), jnp.float32, smallest / len(shards), top_value / len(shards))
        level = level * jnp.repeat(jnp.exp(heights), shape[dim] // parts).reshape((-1,) + (1,) * (len(shape) - 1 - dim))
    return level


def noise(own_key, extent, scale, most, pieces=(), held_as=jnp.bfloat16):
    result = jax.random.normal(own_key, extent, jnp.float32) * scale
    if len(pieces) > 0:
        result = steps_of(own_key, extent, pieces, -0.22, 0.18) * result
    return jnp.clip(result, min=-most, max=most).astype(held_as)


def setup_inputs(seed: int = 0) -> dict:
    splits = jax.random.split(jax.random.key(seed), 4)
    momentum = noise(splits[0], (D, FF), 1.0, 6.0, ((0, 2), (1, 16)))
    gradient = noise(splits[1], (D, FF), 0.5, 4.0, ((0, 2), (1, 16)))
    factor = noise(splits[2], (FF, R), FF ** -0.5, 0.03125, ((0, 16), (1, 2)), jnp.float32)
    return dict(momentum=momentum, gradient=gradient, factor=factor)


decay_rate = 0.95
epsilon = 1e-06

def reference(momentum, gradient, factor):
    blended = (momentum.astype(jnp.float32) + gradient.astype(jnp.float32)).astype(jnp.bfloat16)
    lowered = factor.astype(jnp.bfloat16)
    left_factor = jnp.dot(blended.astype(jnp.float32), lowered.astype(jnp.float32), preferred_element_type=jnp.float32)
    gram_matrix = lax.dot_general(left_factor, left_factor, (((0,), (0,)), ((), ())), precision=lax.Precision.HIGHEST)
    lower_factor = jnp.linalg.cholesky(gram_matrix)
    solved = jax.scipy.linalg.solve_triangular(lower_factor, left_factor.T, lower=True)
    orthonormal = solved.T.astype(jnp.bfloat16)
    right_factor = lax.dot_general(blended.astype(jnp.float32), orthonormal.astype(jnp.float32), (((0,), (0,)), ((), ())), preferred_element_type=jnp.float32)
    inverse = lax.rsqrt(lax.optimization_barrier(jnp.sum(right_factor * right_factor, axis=0)) + epsilon)
    new_factor = right_factor * inverse[None, :]
    product = lax.dot_general(orthonormal.astype(jnp.float32), right_factor.astype(jnp.bfloat16).astype(jnp.float32), (((1,), (1,)), ((), ())), preferred_element_type=jnp.float32)
    new_momentum = (blended.astype(jnp.float32) - (1.0 - decay_rate) * product).astype(jnp.bfloat16)
    stepped = lax.dot_general(orthonormal.astype(jnp.float32), new_factor.astype(jnp.bfloat16).astype(jnp.float32), (((1,), (1,)), ((), ())), preferred_element_type=jnp.float32)
    update = (stepped * jnp.sqrt(jnp.float32(D * FF / R))).astype(jnp.bfloat16)
    return (new_momentum, new_factor, update)
```

```python
import jax
import jax.numpy as jnp
from jax import lax
from jax.experimental import pallas as pl
from jax.experimental.pallas import tpu as pltpu
from jax.sharding import PartitionSpec as P

decay_rate = 0.95
epsilon = 1e-06
BLOCK = 128


def inverse_kernel(gram_ref, out_ref, state):
    rank = gram_ref.shape[0]
    rows = lax.broadcasted_iota(jnp.int32, (rank, rank), 0)
    columns = lax.broadcasted_iota(jnp.int32, (rank, rank), 1)
    state[:, :rank] = gram_ref[...]
    state[:, rank:] = (rows == columns).astype(jnp.float32)
    r_in = lax.broadcasted_iota(jnp.int32, (BLOCK, BLOCK), 0)
    c_in = lax.broadcasted_iota(jnp.int32, (BLOCK, BLOCK), 1)
    wide = lax.broadcasted_iota(jnp.int32, (BLOCK, rank), 1)

    @pl.loop(0, rank // BLOCK)
    def _(b):
        at = pl.multiple_of(b * BLOCK, BLOCK)
        a = state[pl.ds(at, BLOCK), pl.ds(at, BLOCK)]
        v = (r_in == c_in).astype(jnp.float32)
        for j in range(BLOCK - 1):
            lo = (j + 1) // 8 * 8
            top = a[lo:, :]
            scale = 1.0 / a[j : j + 1, j : j + 1]
            factor = jnp.where(r_in[lo:, :1] > j, top[:, j : j + 1] * scale, 0.0)
            new_a = top - factor * a[j : j + 1, :]
            new_v = v[lo:, :] - factor * v[j : j + 1, :]
            a = new_a if lo == 0 else jnp.concatenate([a[:lo], new_a], axis=0)
            v = new_v if lo == 0 else jnp.concatenate([v[:lo], new_v], axis=0)
        diagonal = jnp.sum(jnp.where(r_in == c_in, a, 0.0), axis=1, keepdims=True)
        block_inverse = v * (1.0 / jnp.sqrt(diagonal))
        solved = jnp.dot(
            block_inverse,
            state[pl.ds(at, BLOCK), :],
            precision=lax.Precision.HIGHEST,
            preferred_element_type=jnp.float32,
        )
        out_ref[pl.ds(at, BLOCK), :] = solved[:, rank:]
        lower = jnp.where(wide >= at + BLOCK, solved[:, :rank], 0.0)
        state[...] = state[...] - lax.dot_general(
            lower,
            solved,
            (((0,), (0,)), ((), ())),
            precision=lax.Precision.HIGHEST,
            preferred_element_type=jnp.float32,
        )


def inverse_of_lower(gram):
    rank = gram.shape[0]
    return pl.pallas_call(
        inverse_kernel,
        out_shape=jax.ShapeDtypeStruct((rank, rank), jnp.float32),
        in_specs=[pl.BlockSpec(memory_space=pltpu.VMEM)],
        out_specs=pl.BlockSpec(memory_space=pltpu.VMEM),
        scratch_shapes=[pltpu.VMEM((rank, 2 * rank), jnp.float32)],
        compiler_params=pltpu.CompilerParams(vmem_limit_bytes=32 << 20),
        cost_estimate=pl.CostEstimate(flops=40_000_000_000, bytes_accessed=2 << 20, transcendentals=0),
    )(gram)


def butterfly(value, axis, size):
    if size & (size - 1):
        return lax.psum(value, axis)
    step = 1
    while step < size:
        value = value + lax.ppermute(value, axis, [(i, i ^ step) for i in range(size)])
        step *= 2
    return value


def on_device(halves, spread, momentum, gradient, factor):
    whole_rows = momentum.shape[0] * halves
    whole_columns = momentum.shape[1] * spread
    own_rank = factor.shape[1]
    rank = own_rank * halves
    place = lax.axis_index("fsdp")
    swap = [(0, 1), (1, 0)]

    blended = (momentum.astype(jnp.float32) + gradient.astype(jnp.float32)).astype(jnp.bfloat16)
    lowered = factor.astype(jnp.bfloat16)

    def summed_rows(columns):
        part = jnp.dot(blended, columns, preferred_element_type=jnp.float32).astype(jnp.bfloat16)
        return lax.psum_scatter(part, "tensor", scatter_dimension=0, tiled=True)

    if halves == 2:
        other = lax.ppermute(lowered, "fsdp", swap)
        mine = summed_rows(lowered)
        theirs = summed_rows(other)
        rows = jnp.where(
            place == 0,
            jnp.concatenate([mine, theirs], axis=1),
            jnp.concatenate([theirs, mine], axis=1),
        )
    else:
        rows = summed_rows(lax.all_gather(lowered, "fsdp", axis=1, tiled=True))

    gram = lax.psum(
        lax.dot_general(rows, rows, (((0,), (0,)), ((), ())), preferred_element_type=jnp.float32),
        ("fsdp", "tensor"),
    )
    left = lax.all_gather(rows, "tensor", axis=0, tiled=True)
    lower_inverse = inverse_of_lower(gram)
    high = lower_inverse.astype(jnp.bfloat16)
    low = (lower_inverse - high.astype(jnp.float32)).astype(jnp.bfloat16)
    across = (((1,), (1,)), ((), ()))
    orthonormal = (
        lax.dot_general(left, high, across, preferred_element_type=jnp.float32)
        + lax.dot_general(left, low, across, preferred_element_type=jnp.float32)
    ).astype(jnp.bfloat16)

    share = lax.dot_general(
        orthonormal, blended, (((0,), (0,)), ((), ())), preferred_element_type=jnp.float32
    ).astype(jnp.bfloat16)
    if halves == 2:
        right = share.astype(jnp.float32) + lax.ppermute(share, "fsdp", swap).astype(jnp.float32)
    else:
        right = lax.psum(share, "fsdp").astype(jnp.float32)
    square_sums = butterfly(jnp.sum(right * right, axis=1), "tensor", spread)
    inverse = lax.rsqrt(square_sums + epsilon)
    normal = right * inverse[:, None]
    own_factor = lax.dynamic_slice_in_dim(normal, place * own_rank, own_rank, axis=0).T
    product = jnp.dot(orthonormal, right.astype(jnp.bfloat16), preferred_element_type=jnp.float32)
    new_momentum = (blended.astype(jnp.float32) - (1.0 - decay_rate) * product).astype(jnp.bfloat16)
    stepped = jnp.dot(orthonormal, normal.astype(jnp.bfloat16), preferred_element_type=jnp.float32)
    scale = jnp.sqrt(jnp.float32(whole_rows * whole_columns / rank))
    update = (stepped * scale).astype(jnp.bfloat16)
    return (new_momentum, own_factor, update)


def solution(mesh):
    halves, spread = mesh.shape["fsdp"], mesh.shape["tensor"]

    def body(momentum, gradient, factor):
        return on_device(halves, spread, momentum, gradient, factor)

    return jax.shard_map(
        body,
        mesh=mesh,
        in_specs=(P("fsdp", "tensor"), P("fsdp", "tensor"), P("tensor", "fsdp")),
        out_specs=(P("fsdp", "tensor"), P("tensor", "fsdp"), P("fsdp", "tensor")),
        check_vma=False,
    )
```
